128 devices in a mesh: outer: 8 (over z, x_lo), inner: 16 (over y, x_hi, core).
Axes of the slice: x: 4 (x_hi: 2, x_lo: 2; x = x_hi * 2 + x_lo), y: 4, z: 4, core: 2. Of those that a mesh axis runs over, the one named last changes fastest.
Arguments:
- query_proj: bfloat16 [8192, 8192], P(('outer', 'inner')), may hold values from -8 to 8
- key_proj: bfloat16 [8192, 512], P(('outer', 'inner')), may hold values from -8 to 8
- value_proj: bfloat16 [8192, 512], P(('outer', 'inner')), may hold values from -6 to 6
- positions: int32 [8192], P(('outer', 'inner')), may hold values from 0 to 8191, each once
Outputs:
- attended: bfloat16 [8192, 8192], P(('outer', 'inner'))
The draws below stay inside these ranges and needn't reach their ends.
Inputs may be any that keep to these rules, and one draw needn't show every extreme that they name: `positions`: each position from 0 to 8191 appears exactly once.
All inputs are finite; a program needn't handle non-finite values.
Results may differ from the reference program's by a relative error of at most 0.005.
Values may be sent and summed in bfloat16 or wider, within the bound.
No kernel may reach another device: no remote copies, remote signals or barrier semaphores. Data moves between devices by JAX's collectives and lax.ppermute only.
A program may use at most 64 MiB of HBM per device.

```python
import math
import jax
import jax.numpy as jnp
from jax import lax

HEADS = 64
KV_HEADS = 4
HEAD_WIDTH = 128
TOKENS = 8192


def draw_query_proj(key, part):
    shape_rows = TOKENS
    width = HEADS * HEAD_WIDTH
    sub_key = jax.random.fold_in(key, 1)
    base = 1.4 * jax.random.normal(sub_key, (shape_rows, width), jnp.float32)
    return jnp.clip(base, -8.0, 8.0).astype(jnp.bfloat16)


def draw_key_proj(key, part):
    shape_rows = TOKENS
    width = KV_HEADS * HEAD_WIDTH
    sub_key = jax.random.fold_in(key, 2)
    base = 1.4 * jax.random.normal(sub_key, (shape_rows, width), jnp.float32)
    return jnp.clip(base, -8.0, 8.0).astype(jnp.bfloat16)


def block_levels(stream_key, shape, shards, low, high):
    factor_of, own = 1.0, jax.random.fold_in(stream_key, 6)
    for axis_at, blocks in shards:
        heights = jnp.exp(jax.random.uniform(jax.random.fold_in(own, axis_at), (blocks,), jnp.float32, low / len(shards), high / len(shards)))
        factor_of = factor_of * jnp.repeat(heights, shape[axis_at] // blocks).reshape([-1 if axis == axis_at else 1 for axis in range(len(shape))])
    return factor_of


def gaussian(key, dims, scale, bound, shards=(), kind=jnp.bfloat16):
    array = scale * jax.random.normal(key, dims, jnp.float32)
    if shards:
        array = array * block_levels(key, dims, shards, -0.22, 0.18)
    return jnp.clip(array, -bound, bound).astype(kind)


def setup_inputs(seed: int = 0) -> dict:
    key_of = jax.random.split(jax.random.key(seed), 5)
    return {
        "query_proj": draw_query_proj(jax.random.fold_in(key_of[4], 71), 0),
        "key_proj": draw_key_proj(jax.random.fold_in(key_of[4], 71), 0),
        "value_proj": gaussian(key_of[2], (TOKENS, KV_HEADS * HEAD_WIDTH), 1.0, 6.0, ((0, 128),)),
        "positions": jax.random.permutation(key_of[3], TOKENS).astype(jnp.int32),
    }


def reference(query_proj, key_proj, value_proj, positions):
    all_tokens = query_proj.shape[0]
    group_size = HEADS // KV_HEADS
    scaling = 1.0 / math.sqrt(HEAD_WIDTH)
    query_view = query_proj.reshape(all_tokens, KV_HEADS, group_size, HEAD_WIDTH)
    key_heads = key_proj.reshape(all_tokens, KV_HEADS, HEAD_WIDTH).transpose(1, 0, 2).astype(jnp.float32)
    value_heads = value_proj.reshape(all_tokens, KV_HEADS, HEAD_WIDTH).transpose(1, 0, 2).astype(jnp.float32)
    block_rows = math.gcd(all_tokens, 512)
    block_count = all_tokens // block_rows

    def one_block(block_index):
        first_row = (block_index * block_rows).astype(jnp.int32)
        query_block = lax.dynamic_slice_in_dim(query_view, first_row, block_rows, 0).astype(jnp.float32)
        query_pos = lax.dynamic_slice_in_dim(positions, first_row, block_rows, 0)
        visible = positions[None, :] <= query_pos[:, None]

        def one_head(operands):
            query_head, key_head, value_head = operands
            scores = jnp.einsum('qgd,kd->gqk', query_head, key_head) * scaling
            row_top = lax.optimization_barrier(jnp.max(jnp.where(visible[None], scores, -1e+30), axis=2))
            softmax_weights = jnp.where(visible[None], jnp.exp(scores - row_top[:, :, None]), 0.0)
            row_total_sum = lax.optimization_barrier(jnp.sum(softmax_weights, axis=2))
            rounded = softmax_weights.astype(jnp.bfloat16).astype(jnp.float32)
            weighted = jnp.einsum('gqk,kd->gqd', rounded, value_head)
            return weighted / row_total_sum[:, :, None]
        outputs = lax.map(one_head, (query_block.transpose(1, 0, 2, 3), key_heads, value_heads))
        return outputs.transpose(2, 0, 1, 3).reshape(block_rows, HEADS * HEAD_WIDTH).astype(jnp.bfloat16)
    blocks = lax.map(one_block, jnp.arange(block_count, dtype=jnp.int32))
    return blocks.reshape(all_tokens, HEADS * HEAD_WIDTH)
```

```python
import functools, math
import jax
import jax.numpy as jnp
from jax import lax
from jax.experimental import pallas as pl
from jax.sharding import Mesh
from jax.sharding import PartitionSpec as P
from jax.experimental.pallas import tpu as pltpu

HEAD_WIDTH = 128
VMEM = pltpu.VMEM
LOW_TOP = -1e29
MASKED = -1e30
QT = 16
KT = 16

def f32(x): return x.astype(jnp.float32)
def b16(x): return x.astype(jnp.bfloat16)

def order_kernel(r0, r1, r2, r3, key_ref, val_ref, fwd_ref, back_ref):
    r = jnp.concatenate([r0[...], r1[...], r2[...], r3[...]], axis=0)
    n = r.shape[0]
    digits = f32(r[:, 256:384])
    pcol = digits[:, 0:1] * 64.0 + digits[:, 1:2]
    dt = digits.T
    prow = dt[0:1, :] * 64.0 + dt[1:2, :]
    below = jnp.where(pcol < prow, 1.0, 0.0)
    rank_row = jnp.sum(below, axis=0, keepdims=True)
    above = jnp.where(prow < pcol, 1.0, 0.0)
    rank_col = jnp.sum(above, axis=1, keepdims=True)
    rows = f32(lax.broadcasted_iota(jnp.int32, (n, n), 0))
    cols = f32(lax.broadcasted_iota(jnp.int32, (n, n), 1))
    fwd = b16(jnp.where(rows == rank_row, 1.0, 0.0))
    fwd_ref[...] = fwd
    back_ref[...] = b16(jnp.where(cols == rank_col, 1.0, 0.0))
    srt = jnp.dot(fwd, r, preferred_element_type=jnp.float32)
    key_ref[0:n, :] = b16(srt[:, 0:128])
    val_ref[...] = b16(srt[:, 128:256])
    st = srt[:, 256:384].T
    parts = [st[d:d + 1, 128 * c:128 * (c + 1)] for d in (0, 1) for c in range(n // 128)]
    parts.append(jnp.zeros((16 - len(parts), 128), jnp.float32))
    key_ref[n:n + 16, :] = b16(jnp.concatenate(parts, axis=0))

def order(pieces):
    n = 4 * pieces[0].shape[0]
    return pl.pallas_call(
        order_kernel,
        out_shape=(jax.ShapeDtypeStruct((n + 16, 128), jnp.bfloat16),
                   jax.ShapeDtypeStruct((n, 128), jnp.bfloat16),
                   jax.ShapeDtypeStruct((n, n), jnp.bfloat16),
                   jax.ShapeDtypeStruct((n, n), jnp.bfloat16)),
        name="order",
    )(*pieces)

def block_positions(dig, n):
    c = n // 128
    hi = jnp.concatenate([dig[:, i, :] for i in range(c)], axis=1)
    lo = jnp.concatenate([dig[:, c + i, :] for i in range(c)], axis=1)
    return hi, lo

def attend_kernel(heads, n, key_at, val_at, *refs):
    blocks = len(key_at)
    nk = 1 + max(a for a, _ in key_at)
    nv = 1 + max(a for a, _ in val_at)
    q0, q1, q2, q3, own_ref, fwd_ref, back_ref = refs[:7]
    key_refs, val_refs = refs[7:7 + nk], refs[7 + nk:7 + nk + nv]
    (out_ref, vt_ref, kp_ref, qs_ref, os_ref, qp_ref, acc_ref, qhl_ref, s0_ref, s1_ref, p0_ref, p1_ref, bounds) = refs[7 + nk + nv:]
    def key_rows(start, count):
        return [key_refs[a][j, pl.ds(start, count), :] for a, j in key_at]
    def val_rows(start, count):
        return [val_refs[a][j, pl.ds(start, count), :] for a, j in val_at]
    dv = HEAD_WIDTH
    ntile = n // KT
    qtiles = n // QT
    width = KT * blocks
    qw = QT * heads
    scale = math.log2(math.e) / math.sqrt(dv)
    for c in range(heads * dv // 512):
        qs_ref[:, 512 * c:512 * (c + 1)] = b16(jnp.dot(fwd_ref[...], jnp.concatenate([q[:, 512 * c:512 * (c + 1)] for q in (q0, q1, q2, q3)], axis=0), preferred_element_type=jnp.float32))
    hi, lo = block_positions(f32(jnp.stack(key_rows(n, 16))), n)
    kpos = hi * 64.0 + lo
    kcol = kpos.T
    for t in range(ntile):
        slab = kcol[KT * t:KT * (t + 1), :]
        for b in range(blocks):
            kp_ref[t, KT * b:KT * (b + 1), :] = jnp.broadcast_to(slab[:, b:b + 1], (KT, 128))
        v = jnp.concatenate(val_rows(KT * t, KT), axis=0)
        vt_ref[t, 0:dv, :] = b16(f32(v).T)
        vt_ref[t, dv:dv + 16, :] = jnp.ones((16, width), jnp.bfloat16)
    low = jnp.min(kpos, axis=0, keepdims=True)
    high = jnp.max(kpos, axis=0, keepdims=True)
    lane = lax.broadcasted_iota(jnp.int32, (1, n), 1)
    own_hi, own_lo = block_positions(f32(own_ref[n:n + 16, :])[None], n)
    tile_of = lax.broadcasted_iota(jnp.int32, (qtiles, n), 1) // QT
    mine = tile_of == lax.broadcasted_iota(jnp.int32, (qtiles, n), 0)
    rep = b16(jnp.where(lax.broadcasted_iota(jnp.int32, (n, qw), 0) % QT == lax.broadcasted_iota(jnp.int32, (n, qw), 1) % QT, 1.0, 0.0))
    mh = b16(jnp.where(mine, own_hi, 0.0))
    ml = b16(jnp.where(mine, own_lo, 0.0))
    qp_ref[0:qtiles, :] = (jnp.dot(mh, rep, preferred_element_type=jnp.float32) * 64.0
                   + jnp.dot(ml, rep, preferred_element_type=jnp.float32))
    own = own_hi * 64.0 + own_lo
    for i in range(qtiles):
        first = own[:, QT * i:QT * i + 1]
        last = own[:, QT * i + QT - 1:QT * i + QT]
        seen = jnp.where((lane % KT == 0) & (low <= last), 1.0, 0.0)
        full = jnp.where((lane % KT == KT - 1) & (high <= first), 1.0, 0.0)
        bounds[0, i] = jnp.sum(full).astype(jnp.int32)
        bounds[1, i] = jnp.sum(seen).astype(jnp.int32)

    for i in range(qtiles):
        q = f32(qs_ref[QT * i:QT * (i + 1), :])
        qstack = jnp.concatenate([q[:, dv * h:dv * (h + 1)] for h in range(heads)], axis=0)
        qt = qstack.T * scale
        qhi = b16(qt)
        qhl_ref[i, 0:dv, :] = qhi
        qhl_ref[i, dv:2 * dv, :] = b16(qt - f32(qhi))
    acc_ref[...] = jnp.zeros_like(acc_ref)
    p1_ref[...] = jnp.zeros_like(p1_ref)

    def score(i, t, s_ref):
        k = jnp.concatenate(key_rows(pl.multiple_of(t * KT, KT), KT), axis=0)
        kk = jnp.concatenate([k, k], axis=1)
        s_ref[...] = jnp.dot(kk, qhl_ref[i], preferred_element_type=jnp.float32)

    def soft(i, t, top, s_ref, p_ref):
        kp = kp_ref[t]
        vis = jnp.concatenate([kp] * (qw // 128), axis=1) <= qp_ref[pl.ds(i, 1), :]
        s = jnp.where(vis, s_ref[...], MASKED)
        top = jnp.where(t == 0, LOW_TOP, top)
        new = jnp.maximum(top, jnp.max(s, axis=0, keepdims=True))
        p_ref[...] = b16(jnp.exp2(s - new))
        return new, jnp.where(t == 0, 0.0, jnp.exp2(top - new))

    def gather(i, t, alpha, p_ref):
        pv = jnp.dot(vt_ref[t], p_ref[...], preferred_element_type=jnp.float32)
        acc_ref[i] = acc_ref[i] * alpha + pv

    def after(i, t):
        more = t + 1 < bounds[1, jnp.minimum(i, qtiles - 1)]
        return jnp.where(i >= qtiles, i, jnp.where(more, i, i + 1)), jnp.where(i >= qtiles, 0, jnp.where(more, t + 1, 0))

    score(0, 0, s0_ref)
    total = bounds[1, 0]
    for i in range(1, qtiles):
        total = total + bounds[1, i]

    def pair(w, carry):
        pi, pt, ci, ct, top, alpha = carry
        ni, nt = after(ci, ct)
        score(ni, nt, s1_ref)
        gather(pi, pt, alpha, p1_ref)
        top, alpha = soft(ci, ct, top, s0_ref, p0_ref)
        ei, et = after(ni, nt)
        score(ei, et, s0_ref)
        gather(ci, ct, alpha, p0_ref)
        top, alpha = soft(ni, nt, top, s1_ref, p1_ref)
        return ni, nt, ei, et, top, alpha

    z = jnp.int32(0)
    pi, pt, ci, ct, top, alpha = lax.fori_loop(0, (total + 1) // 2, pair, (
        jnp.int32(qtiles), z, z, z, jnp.full((1, qw), LOW_TOP, jnp.float32), jnp.zeros((1, qw), jnp.float32)))
    gather(pi, pt, alpha, p1_ref)
    for i in range(qtiles):
        o = acc_ref[i, 0:dv, :] / acc_ref[i, dv:dv + 1, :]
        ot = o.T
        os_ref[QT * i:QT * (i + 1), :] = b16(jnp.concatenate([ot[QT * h:QT * (h + 1), :] for h in range(heads)], axis=1))

    for c in range(heads * dv // 512):
        out_ref[:, 512 * c:512 * (c + 1)] = b16(jnp.dot(back_ref[...], os_ref[:, 512 * c:512 * (c + 1)], preferred_element_type=jnp.float32))

def attend(qs, own, fwd, back, key_arrays, val_arrays, key_at, val_at):
    n, hw = fwd.shape[0], qs[0].shape[1]
    heads = hw // HEAD_WIDTH
    blocks = len(key_at)
    qw = QT * heads
    ntile = n // KT
    return pl.pallas_call(
        functools.partial(attend_kernel, heads, n, key_at, val_at),
        out_shape=jax.ShapeDtypeStruct((n, hw), jnp.bfloat16),
        scratch_shapes=[
            VMEM((ntile, HEAD_WIDTH + 16, KT * blocks), jnp.bfloat16),
            VMEM((ntile, KT * blocks, 128), jnp.float32),
            VMEM((n, hw), jnp.bfloat16),
            VMEM((n, hw), jnp.bfloat16),
            VMEM((n // QT + 8, qw), jnp.float32),
            VMEM((n // QT + 1, HEAD_WIDTH + 16, qw), jnp.float32),
            VMEM((n // QT + 1, 2 * HEAD_WIDTH, qw), jnp.bfloat16),
            VMEM((KT * blocks, qw), jnp.float32),
            VMEM((KT * blocks, qw), jnp.float32),
            VMEM((KT * blocks, qw), jnp.bfloat16),
            VMEM((KT * blocks, qw), jnp.bfloat16),
            pltpu.SMEM((2, n // QT), jnp.int32),
        ],
        compiler_params=pltpu.CompilerParams(vmem_limit_bytes=48 * 1024 * 1024),
        name="attend",
        cost_estimate=pl.CostEstimate(flops=2 * 2 * n * heads * blocks * n * HEAD_WIDTH, bytes_accessed=8 << 20, transcendentals=n * heads * blocks * n),
    )(*qs, own, fwd, back, *key_arrays, *val_arrays)

AXES = ("z", "xlo", "y", "xhi", "c")
XAXES = ("xlo", "xhi")

def x_index(x):
    return (x % 2) * 2 + x // 2

def shift(value, axis, by):
    if axis == "x":
        return lax.ppermute(value, XAXES, [(x_index(i), x_index((i + by) % 4)) for i in range(4)])
    size = lax.axis_size(axis)
    return lax.ppermute(value, axis, [(i, (i + by) % size) for i in range(size)])

def gather_row(value, axis):
    return jnp.stack([value, shift(value, axis, 1), shift(value, axis, 3), shift(value, axis, 2)])

def gather_wide(value, axis):
    right, left = shift(value, axis, 1), shift(value, axis, 3)
    far_a, far_b = shift(right[:2], axis, 1), shift(left[2:], axis, 3)
    return jnp.concatenate([value, right, left, far_a, far_b])

def body(query_proj, key_proj, value_proj, positions):
    rows, width = query_proj.shape
    me = lax.axis_index("y")
    group = width // 4
    digits = jnp.stack([positions // 64, positions % 64], axis=1).astype(jnp.bfloat16)
    digits = jnp.pad(digits, ((0, 0), (0, HEAD_WIDTH - 2)))
    pack = jnp.stack([jnp.concatenate([key_proj[:, HEAD_WIDTH * h:HEAD_WIDTH * (h + 1)],
                                       value_proj[:, HEAD_WIDTH * h:HEAD_WIDTH * (h + 1)], digits], axis=1) for h in range(4)])
    def for_peer(by):
        return lax.dynamic_index_in_dim(pack, (me + by) % 4, 0, keepdims=False)
    pieces = [for_peer(0)] + [shift(for_peer(by), "y", by) for by in (1, 2, 3)]
    def q_for(by):
        return lax.dynamic_slice_in_dim(query_proj, ((me + by) % 4) * group, group, 1)
    qs = [q_for(0)] + [shift(q_for(by), "y", by) for by in (1, 2, 3)]
    key, val, fwd, back = order(pieces)
    key_all = gather_wide(gather_row(key, "z"), "x")
    val_all = gather_wide(gather_row(val, "x"), "z")
    key_twin, val_twin = shift(key_all, "c", 1), shift(val_all, "c", 1)
    key_at, val_at = [], []
    for core in range(2):
        for dx in range(4):
            for dz in range(4):
                key_at.append((core, 4 * dx + dz))
                val_at.append((core, 4 * dz + dx))
    out = attend(qs, key, fwd, back, [key_all, key_twin], [val_all, val_twin], key_at, val_at)
    back_home = [out[0:rows]] + [shift(out[rows * by:rows * (by + 1)], "y", 4 - by) for by in (1, 2, 3)]
    stacked = jnp.stack(back_home)
    result = jnp.concatenate([lax.dynamic_index_in_dim(stacked, (h - me) % 4, 0, keepdims=False) for h in range(4)], axis=1)
    return result

def solution(mesh):
    finer = Mesh(mesh.devices.reshape(4, 2, 4, 2, 2), AXES)
    return jax.shard_map(
        body,
        mesh=finer,
        in_specs=(P(AXES, None), P(AXES, None), P(AXES, None), P(AXES)),
        out_specs=P(AXES, None),
        check_vma=False,
    )
```
